8 devices in a mesh: part: 1 (over z), col: 2 (over y), row: 4 (over x, core).
Axes of the slice: x: 2, y: 2, z: 1, core: 2. Of those that a mesh axis runs over, the one named last changes fastest.
Arguments:
- mat_one: float32 [40, 128, 5120], P(('part', 'row'), None, 'col')
- mat_two: float32 [40, 128, 5120], P(('part', 'row'), None, 'col')
Outputs:
- output 1: float32 [40, 128, 5120], P(('part', 'row'), None, 'col')
- output 2: float32 [40, 128, 5120], P(('part', 'row'), None, 'col')
All inputs are finite; a program needn't handle non-finite values.
Results may differ from the reference program's by a relative error of at most 0.001.
Values sent between devices are 32-bit elements.
A program may use at most 1 GiB of HBM per device.

```python
import jax
import jax.numpy as jnp
from jax import lax

N = 5120
NB = 128
ROWS = 4
COLS = 2
BLOCKS = N // NB
RANK = N // 4


def to_cyclic(natural):
    by_rows = natural.reshape(BLOCKS // ROWS, ROWS, NB, N).transpose(1, 0, 2, 3)
    by_cols = by_rows.reshape(BLOCKS, NB, BLOCKS // COLS, COLS, NB).transpose(0, 1, 3, 2, 4)
    return by_cols.reshape(BLOCKS, NB, N)


def from_cyclic(stored):
    by_rows = stored.reshape(ROWS, BLOCKS // ROWS, NB, N).transpose(1, 0, 2, 3).reshape(N, N)
    by_cols = by_rows.reshape(N, COLS, BLOCKS // COLS, NB).transpose(0, 2, 1, 3)
    return by_cols.reshape(N, N)


def make_spd(draw_key):
    factor = jax.random.normal(draw_key, (N, RANK), jnp.float32)
    gram_mat = jnp.dot(factor, factor.T, precision=lax.Precision.HIGHEST, preferred_element_type=jnp.float32) / RANK
    gram_mat = 0.5 * (gram_mat + gram_mat.T)
    return to_cyclic(gram_mat + jnp.eye(N, dtype=jnp.float32))


def setup_inputs(seed: int = 0, part: int = 0) -> dict:
    part_key = jax.random.fold_in(jax.random.key(seed), part)
    key_one, key_two = jax.random.split(part_key)
    return {"mat_one": make_spd(key_one), "mat_two": make_spd(key_two)}


def lower_factor(stored):
    return to_cyclic(jnp.linalg.cholesky(from_cyclic(stored)))


def reference(mat_one, mat_two):
    return (lower_factor(mat_one), lower_factor(mat_two))
```

```python
import functools

import jax
import jax.numpy as jnp
from jax import lax
from jax.experimental import pallas as pl
from jax.experimental.pallas import tpu as pltpu
from jax.sharding import PartitionSpec as P

PRECISE = lax.Precision.HIGHEST
NB = 128
VMEM_SPEC = pl.BlockSpec(memory_space=pltpu.VMEM)
HBM_SPEC = pl.BlockSpec(memory_space=pltpu.HBM)
SMEM_SPEC = pl.BlockSpec(memory_space=pltpu.SMEM)
LIMIT = 60 * 1024 * 1024


def nt(a, b):
    return lax.dot_general(a, b, (((1,), (1,)), ((), ())), precision=PRECISE, preferred_element_type=jnp.float32)


def factor_128(block):
    lane = lax.broadcasted_iota(jnp.int32, (8, 128), 1)
    sub = lax.broadcasted_iota(jnp.int32, (8, 128), 0)
    wide = (8, 128)
    rows = [block[8 * q:8 * q + 8, :] for q in range(16)]
    done, diag_parts = [], []
    for p in range(16):
        cur = rows[p]
        lo = 8 * p
        inside = jnp.logical_and(lane >= lo, lane < lo + 8)
        cols = [jnp.broadcast_to(cur[:, lo + j:lo + j + 1], wide) for j in range(8)]
        has_next = p < 15
        if has_next:
            nxt = rows[p + 1]
            ncols = [jnp.broadcast_to(nxt[:, lo + j:lo + j + 1], wide) for j in range(8)]
            nxt = jnp.where(inside, 0.0, nxt)
        cur = jnp.where(inside, jnp.where(lane - lo == sub, 1.0, 0.0), cur)
        diag_part = jnp.zeros(wide, jnp.float32)
        for j in range(8):
            pivot = jnp.broadcast_to(cols[j][j:j + 1, :], wide)
            inv_root = lax.rsqrt(pivot)
            lcol = cols[j] * inv_root
            for m in range(j + 1, 8):
                cols[m] = cols[m] - lcol * jnp.broadcast_to(lcol[m:m + 1, :], wide)
            wrow = jnp.broadcast_to(cur[j:j + 1, :], wide) * inv_root
            cur = jnp.where(sub == j, wrow, cur - jnp.where(sub > j, lcol, 0.0) * wrow)
            if has_next:
                ncol = ncols[j] * inv_root
                nxt = nxt - ncol * wrow
                for m in range(j + 1, 8):
                    ncols[m] = ncols[m] - ncol * jnp.broadcast_to(lcol[m:m + 1, :], wide)
            diag_part = jnp.where(jnp.logical_and(lane == lo + j, sub >= j), lcol, diag_part)
        done.append(cur)
        diag_parts.append(diag_part)
        if has_next:
            rows[p + 1] = nxt
        if p < 14:
            flipped = cur.T
            for q in range(p + 2, 16):
                acc = jnp.where(inside, 0.0, rows[q])
                for j in range(8):
                    acc = acc - jnp.broadcast_to(flipped[8 * q:8 * q + 8, j:j + 1], wide) * jnp.broadcast_to(cur[j:j + 1, :], wide)
                rows[q] = acc
    packed = jnp.concatenate(done, axis=0)
    diag8 = jnp.concatenate(diag_parts, axis=0)
    full_lane = lax.broadcasted_iota(jnp.int32, (128, 128), 1) // 8
    full_sub = lax.broadcasted_iota(jnp.int32, (128, 128), 0) // 8
    inverse = jnp.where(full_lane <= full_sub, packed, 0.0)
    upper = jnp.where(full_lane > full_sub, packed, 0.0)
    return upper.T + diag8, inverse

def chain_kernel(s_ref, l_ref, inv_ref, work):
    work[...] = s_ref[...]
    n = s_ref.shape[0] // 128
    rowb = lax.broadcasted_iota(jnp.int32, (n * 128, 128), 0) // 128
    def step(k, _):
        lo = pl.multiple_of(k * 128, 128)
        fac, inv = factor_128(work[pl.ds(lo, 128), pl.ds(lo, 128)])
        inv_ref[pl.ds(lo, 128), :] = inv
        col = nt(work[:, pl.ds(lo, 128)], inv)
        col = jnp.where(rowb > k, col, 0.0)
        l_ref[:, pl.ds(lo, 128)] = col
        l_ref[pl.ds(lo, 128), pl.ds(lo, 128)] = fac
        work[...] = work[...] - nt(col, col)
        return 0
    lax.fori_loop(0, n, step, 0)


def shape_of(*dims):
    return jax.ShapeDtypeStruct(dims, jnp.float32)


def cost(flops):
    return pl.CostEstimate(flops=int(flops), bytes_accessed=1 << 20, transcendentals=0)


def chain(s):
    n = s.shape[0]
    return pl.pallas_call(
        chain_kernel,
        out_shape=(shape_of(n, n), shape_of(n, NB)),
        in_specs=[VMEM_SPEC],
        out_specs=(VMEM_SPEC,) * 2,
        scratch_shapes=[pltpu.VMEM((n, n), jnp.float32)],
        cost_estimate=cost(2.5e9),
        name="chain",
    )(s)


def solve_kernel(rows_n, rest, ahead, *refs):
    me_ref, lss_ref, inv_ref = refs[:3]
    sub_refs = refs[3:3 + rows_n]
    next_refs = refs[3 + rows_n:3 + 2 * rows_n]
    pos = 3 + 2 * rows_n
    if ahead:
        own_ref, w_ref, lown_ref, sb_ref, wout_ref, panel = refs[pos:]
    else:
        lown_ref, sb_ref, panel = refs[pos:]
    me = me_ref[0]
    wide = rows_n * NB
    for k in range(rows_n):
        lo = pl.multiple_of(lax.bitwise_xor(me, k) * NB, NB)
        panel[pl.ds(lo, NB), :] = sub_refs[k][...]
        sb_ref[pl.ds(lo, NB), :] = next_refs[k][...]
    if ahead:
        panel[wide:, :] = own_ref[NB:, :]
    for k in range(rows_n):
        cols = slice(k * NB, (k + 1) * NB)
        solved = nt(panel[:, cols], inv_ref[cols, :])
        panel[:, cols] = solved
        if k + 1 < rows_n:
            panel[:, (k + 1) * NB:] = panel[:, (k + 1) * NB:] - nt(solved, lss_ref[(k + 1) * NB:, cols])
    sub = panel[:wide, :]
    sb_ref[...] = sb_ref[...] - nt(sub, sub)
    lown_ref[:NB, :] = panel[pl.ds(pl.multiple_of(me * NB, NB), NB), :]
    if ahead:
        lown_ref[NB:, :] = panel[wide:, :]
        wout_ref[...] = w_ref[...] - nt(panel[wide:, :], sub)


def solve(me, lss, inv, own, sub_rel, next_rel, w_rest):
    rows_n = len(sub_rel)
    wide = rows_n * NB
    rest = w_rest.shape[0] if w_rest is not None else 0
    ahead = rest > 0
    args = [me, lss, inv, *sub_rel, *next_rel]
    outs = [shape_of(NB + rest, wide), shape_of(wide, wide)]
    if ahead:
        args += [own, w_rest]
        outs.append(shape_of(rest, wide))
    return pl.pallas_call(
        functools.partial(solve_kernel, rows_n, rest, ahead),
        out_shape=tuple(outs),
        in_specs=[SMEM_SPEC] + [VMEM_SPEC] * (len(args) - 1),
        out_specs=(VMEM_SPEC,) * len(outs),
        scratch_shapes=[pltpu.VMEM((wide + rest, wide), jnp.float32)],
        compiler_params=pltpu.CompilerParams(vmem_limit_bytes=LIMIT),
        cost_estimate=cost(2 * (wide + rest) * wide * wide * 2),
        name="solve",
    )(*args)


def update_kernel(rows_n, terms, height, *refs):
    me_ref, w_ref = refs[:2]
    count = len(terms)
    left_refs = refs[2:2 + count]
    right_refs = refs[2 + count:2 + count + count * rows_n]
    out_ref, left, right, sem = refs[2 + count + count * rows_n:]
    me = me_ref[0]
    wide = rows_n * NB
    pending = []
    for i, (left_lo, right_los) in enumerate(terms):
        copies = [pltpu.make_async_copy(left_refs[i].at[pl.ds(left_lo, height), :], left.at[i], sem.at[i, rows_n])]
        for k in range(rows_n):
            lo = pl.multiple_of(lax.bitwise_xor(me, k) * NB, NB)
            copies.append(pltpu.make_async_copy(
                right_refs[i * rows_n + k].at[pl.ds(right_los[k], NB), :], right.at[i, pl.ds(lo, NB), :], sem.at[i, k]))
        for copy in copies:
            copy.start()
        pending.append(copies)
    out_ref[...] = w_ref[...]
    for i in range(count):
        for copy in pending[i]:
            copy.wait()
        out_ref[...] = out_ref[...] - nt(left[i], right[i])


def update(me, w, lefts, rights, terms):
    rows_n = len(rights[0])
    wide = rows_n * NB
    height = w.shape[0]
    count = len(terms)
    args = [me, w, *lefts, *[piece for group in rights for piece in group]]
    return pl.pallas_call(
        functools.partial(update_kernel, rows_n, terms, height),
        out_shape=shape_of(height, wide),
        in_specs=[SMEM_SPEC, VMEM_SPEC] + [HBM_SPEC] * (len(args) - 2),
        out_specs=VMEM_SPEC,
        scratch_shapes=[
            pltpu.VMEM((count, height, wide), jnp.float32),
            pltpu.VMEM((count, wide, wide), jnp.float32),
            pltpu.SemaphoreType.DMA((count, rows_n + 1)),
        ],
        compiler_params=pltpu.CompilerParams(vmem_limit_bytes=LIMIT),
        cost_estimate=cost(2 * height * wide * wide * count * 2),
        name="update",
    )(*args)


def tie(first, second):
    return lax.optimization_barrier((first, second))


def factor_pair(mat_one, mat_two, rows_n, cols_n):
    row_blocks, block_len, local_width = mat_one.shape
    steps = row_blocks
    wide = rows_n * NB
    half = wide // cols_n
    per = half // NB
    my_row = lax.axis_index("row")
    first = lax.axis_index("col") == 0
    me = my_row.astype(jnp.int32).reshape(1)
    swap = [(0, 1), (1, 0)]

    def hop(value, mask):
        return lax.ppermute(value, "row", [(i, i ^ mask) for i in range(rows_n)])

    def gather(value):
        far = hop(value, 2)
        return [value, hop(value, 1), far, hop(far, 1)]

    def panel_of(step, row_lo, row_hi):
        cols = slice(step * half, (step + 1) * half)
        piece_one, piece_two = mat_one[row_lo:row_hi, :, cols], mat_two[row_lo:row_hi, :, cols]
        mine = jnp.where(first, piece_one, piece_two)
        got = lax.ppermute(jnp.where(first, piece_two, piece_one), "col", swap)
        even, odd = jnp.where(first, mine, got), jnp.where(first, got, mine)
        parts = []
        for q in range(per):
            parts += [even[..., q * NB:(q + 1) * NB], odd[..., q * NB:(q + 1) * NB]]
        return jnp.concatenate(parts, axis=-1).reshape(-1, wide)

    def in_order(rel):
        picked = []
        for q in range(rows_n):
            value = rel[rows_n - 1]
            for k in range(rows_n - 1):
                value = jnp.where(my_row == (q ^ k), rel[k], value)
            picked.append(value)
        return jnp.concatenate(picked, axis=0)

    sb = in_order(gather(panel_of(0, 0, 1)))
    sub_own = panel_of(0, 1, 2)
    own = jnp.concatenate([sub_own, panel_of(0, 2, steps)], axis=0)
    sub_rel = gather(sub_own)
    diag_own = panel_of(1, 1, 2)
    rest_own = panel_of(1, 2, steps)
    raw = [None, None] + [panel_of(s, s, steps) for s in range(2, steps)]
    lowns, near, later = [], [], []
    out_one, out_two = [], []

    def emit(step, lss_rows, lown):
        full = lss_rows if lown is None else jnp.concatenate([lss_rows, lown], axis=0)
        full = full.reshape(-1, per, cols_n, NB)
        even, odd = full[:, :, 0], full[:, :, 1]
        kept = jnp.where(first, even, odd).reshape(-1, NB, half)
        got = lax.ppermute(jnp.where(first, odd, even).reshape(-1, NB, half), "col", swap)
        pads = ((step, 0), (0, 0), (0, 0))
        out_one.append(jnp.pad(jnp.where(first, kept, got), pads))
        out_two.append(jnp.pad(jnp.where(first, got, kept), pads))

    for step in range(steps):
        lss, inv = chain(sb)
        lss_rows = lax.dynamic_slice(lss, (my_row * NB, 0), (NB, wide))
        if step == steps - 1:
            emit(step, lss_rows, None)
            break
        target = step + 1
        if step >= 1:
            lefts, rights, terms_diag, terms_rest = [], [], [], []
            for past in range(step):
                base = (target - past - 1) * NB
                lefts.append(lowns[past])
                if past == step - 1:
                    rights.append([lowns[past]] + near[past][1:])
                    los = (base,) + (0,) * (rows_n - 1)
                else:
                    rights.append([lowns[past]] + later[past][1:])
                    los = (base,) + ((target - past - 3) * NB,) * (rows_n - 1)
                terms_diag.append((base, los))
                terms_rest.append((base + NB, los))
            panel = raw[target]
            lss, panel = tie(lss, panel)
            diag_own = update(me, panel[:NB], lefts, rights, terms_diag)
            rest_own = None
            if target < steps - 1:
                diag_own, rest_raw = tie(diag_own, panel[NB:])
                rest_own = update(me, rest_raw, lefts, rights, terms_rest)
        next_rel = gather(diag_own)
        if step == steps - 2:
            rest_own = None
        res = solve(me, lss, inv, own, sub_rel, next_rel, rest_own)
        lown, sb = res[0], res[1]
        lowns.append(lown)
        if rest_own is not None:
            own = res[2]
            sub_rel = gather(own[:NB])
        if step <= steps - 3:
            near.append(gather(lown[NB:2 * NB]))
        if step <= steps - 4:
            later.append(gather(lown[2 * NB:]))
        else:
            later.append(None)
        emit(step, lss_rows, lown)
    return jnp.concatenate(out_one, axis=-1), jnp.concatenate(out_two, axis=-1)


def solution(mesh):
    rows_n = mesh.shape["row"]
    cols_n = mesh.shape["col"]
    block_spec = P(("part", "row"), None, "col")

    def run_pair(mat_one, mat_two):
        return factor_pair(mat_one, mat_two, rows_n, cols_n)

    return jax.shard_map(run_pair, mesh=mesh, in_specs=(block_spec, block_spec), out_specs=(block_spec, block_spec), check_vma=False)
```

```python
import functools

import jax
import jax.numpy as jnp
from jax import lax
from jax.experimental import pallas as pl
from jax.experimental.pallas import tpu as pltpu
from jax.sharding import PartitionSpec as P


PRECISE = lax.Precision.HIGHEST
NB = 128
VMEM_SPEC = pl.BlockSpec(memory_space=pltpu.VMEM)
HBM_SPEC = pl.BlockSpec(memory_space=pltpu.HBM)
SMEM_SPEC = pl.BlockSpec(memory_space=pltpu.SMEM)
LIMIT = 60 * 1024 * 1024


def nt(a, b):
    return lax.dot_general(a, b, (((1,), (1,)), ((), ())), precision=PRECISE, preferred_element_type=jnp.float32)


def factor_128(block):
    lane = lax.broadcasted_iota(jnp.int32, (8, 128), 1)
    sub = lax.broadcasted_iota(jnp.int32, (8, 128), 0)
    wide = (8, 128)
    rows = [block[8 * q:8 * q + 8, :] for q in range(16)]
    done, diag_parts = [], []
    for p in range(16):
        cur = rows[p]
        lo = 8 * p
        inside = jnp.logical_and(lane >= lo, lane < lo + 8)
        cols = [jnp.broadcast_to(cur[:, lo + j:lo + j + 1], wide) for j in range(8)]
        has_next = p < 15
        if has_next:
            nxt = rows[p + 1]
            ncols = [jnp.broadcast_to(nxt[:, lo + j:lo + j + 1], wide) for j in range(8)]
            nxt = jnp.where(inside, 0.0, nxt)
        cur = jnp.where(inside, jnp.where(lane - lo == sub, 1.0, 0.0), cur)
        diag_part = jnp.zeros(wide, jnp.float32)
        for j in range(8):
            pivot = jnp.broadcast_to(cols[j][j:j + 1, :], wide)
            inv_root = lax.rsqrt(pivot)
            lcol = cols[j] * inv_root
            for m in range(j + 1, 8):
                cols[m] = cols[m] - lcol * jnp.broadcast_to(lcol[m:m + 1, :], wide)
            wrow = jnp.broadcast_to(cur[j:j + 1, :], wide) * inv_root
            cur = jnp.where(sub == j, wrow, cur - jnp.where(sub > j, lcol, 0.0) * wrow)
            if has_next:
                ncol = ncols[j] * inv_root
                nxt = nxt - ncol * wrow
                for m in range(j + 1, 8):
                    ncols[m] = ncols[m] - ncol * jnp.broadcast_to(lcol[m:m + 1, :], wide)
            diag_part = jnp.where(jnp.logical_and(lane == lo + j, sub >= j), lcol, diag_part)
        done.append(cur)
        diag_parts.append(diag_part)
        if has_next:
            rows[p + 1] = nxt
        if p < 14:
            flipped = cur.T
            for q in range(p + 2, 16):
                acc = jnp.where(inside, 0.0, rows[q])
                for j in range(8):
                    acc = acc - jnp.broadcast_to(flipped[8 * q:8 * q + 8, j:j + 1], wide) * jnp.broadcast_to(cur[j:j + 1, :], wide)
                rows[q] = acc
    packed = jnp.concatenate(done, axis=0)
    diag8 = jnp.concatenate(diag_parts, axis=0)
    full_lane = lax.broadcasted_iota(jnp.int32, (128, 128), 1) // 8
    full_sub = lax.broadcasted_iota(jnp.int32, (128, 128), 0) // 8
    inverse = jnp.where(full_lane <= full_sub, packed, 0.0)
    upper = jnp.where(full_lane > full_sub, packed, 0.0)
    return upper.T + diag8, inverse


def chain_kernel(*refs):
    l_ref, inv_ref, work = refs[-3:]
    n = work.shape[0] // 128
    if len(refs) == 4:
        work[...] = refs[0][...]
    else:
        me, sub = refs[0][0], refs[1][...]
        for k in range(n):
            work[pl.ds(pl.multiple_of(lax.bitwise_xor(me, k) * NB, NB), NB), :] = refs[2 + k][...]
        work[...] = work[...] - nt(sub, sub)
    rowb = lax.broadcasted_iota(jnp.int32, (n * 128, 128), 0) // 128

    def step(k, _):
        lo = pl.multiple_of(k * 128, 128)
        fac, inv = factor_128(work[pl.ds(lo, 128), pl.ds(lo, 128)])
        inv_ref[pl.ds(lo, 128), :] = inv
        col = nt(work[:, pl.ds(lo, 128)], inv)
        col = jnp.where(rowb > k, col, 0.0)
        l_ref[:, pl.ds(lo, 128)] = col
        l_ref[pl.ds(lo, 128), pl.ds(lo, 128)] = fac
        work[...] = work[...] - nt(col, col)
        return 0

    lax.fori_loop(0, n, step, 0)


def shape_of(*dims):
    return jax.ShapeDtypeStruct(dims, jnp.float32)


def cost(flops):
    return pl.CostEstimate(flops=int(flops), bytes_accessed=1 << 20, transcendentals=0)


def chain(*args):
    n = args[-1].shape[1]
    return pl.pallas_call(
        chain_kernel,
        out_shape=(shape_of(n, n), shape_of(n, NB)),
        in_specs=[VMEM_SPEC] if len(args) == 1 else [SMEM_SPEC] + [VMEM_SPEC] * (len(args) - 1),
        out_specs=(VMEM_SPEC,) * 2,
        scratch_shapes=[pltpu.VMEM((n, n), jnp.float32)],
        cost_estimate=cost(2.5e9),
        name="chain",
    )(*args)


def split_store(dst_kept, dst_sent, rows, col, value_of, per):
    for q in range(per):
        kept = pl.multiple_of((2 * q + col) * NB, NB)
        sent = pl.multiple_of((2 * q + 1 - col) * NB, NB)
        dst_kept[rows, q * NB:(q + 1) * NB] = value_of(kept)
        dst_sent[rows, q * NB:(q + 1) * NB] = value_of(sent)


def solve_kernel(rows_n, ahead, far, sub_lo, *refs):
    me_ref, lss_ref, inv_ref = refs[:3]
    sub_refs = refs[3:3 + rows_n]
    rest = list(refs[3 + rows_n:])
    panel = rest.pop()
    if ahead:
        own_ref, w_ref = rest.pop(0), rest.pop(0)
    lown_ref, sub_ref, kept_ref, sent_ref = rest[:4]
    me, col = me_ref[0], me_ref[1]
    wide = rows_n * NB
    per = rows_n // 2
    for k in range(rows_n):
        lo = pl.multiple_of(lax.bitwise_xor(me, k) * NB, NB)
        panel[pl.ds(lo, NB), :] = sub_refs[k][sub_lo:sub_lo + NB, :]
    if ahead:
        panel[wide:, :] = own_ref[NB:, :]
    for k in range(rows_n):
        cols = slice(k * NB, (k + 1) * NB)
        solved = nt(panel[:, cols], inv_ref[cols, :])
        panel[:, cols] = solved
        if k + 1 < rows_n:
            panel[:, (k + 1) * NB:] = panel[:, (k + 1) * NB:] - nt(solved, lss_ref[(k + 1) * NB:, cols])
    sub = panel[:wide, :]
    sub_ref[...] = sub
    mine = pl.ds(pl.multiple_of(me * NB, NB), NB)
    lown_ref[:NB, :] = panel[mine, :]
    split_store(kept_ref, sent_ref, slice(0, NB), col, lambda lo: lss_ref[mine, pl.ds(lo, NB)], per)
    split_store(kept_ref, sent_ref, slice(NB, 2 * NB), col, lambda lo: panel[mine, pl.ds(lo, NB)], per)
    if ahead:
        wout_ref, near_ref = rest[4:6]
        lown_ref[NB:, :] = panel[wide:, :]
        split_store(kept_ref, sent_ref, slice(2 * NB, None), col, lambda lo: panel[wide:, pl.ds(lo, NB)], per)
        wout_ref[...] = w_ref[...] - nt(panel[wide:, :], sub)
        near_ref[:NB, :] = panel[wide:wide + NB, :]
        near_ref[NB:, :] = wout_ref[:NB, :]
        if far:
            rest[6][...] = panel[wide + NB:, :]


def solve(me, lss, inv, own, sub_rel, sub_lo, w_rest):
    rows_n = len(sub_rel)
    wide = rows_n * NB
    rest = w_rest.shape[0] if w_rest is not None else 0
    ahead, far = rest > 0, rest > NB
    args = [me, lss, inv, *sub_rel]
    outs = [shape_of(NB + rest, wide), shape_of(wide, wide)] + [shape_of(2 * NB + rest, wide // 2)] * 2
    if ahead:
        args += [own, w_rest]
        outs += [shape_of(rest, wide), shape_of(2 * NB, wide)]
        if far:
            outs.append(shape_of(rest - NB, wide))
    return pl.pallas_call(
        functools.partial(solve_kernel, rows_n, ahead, far, sub_lo),
        out_shape=tuple(outs),
        in_specs=[SMEM_SPEC] + [VMEM_SPEC] * (len(args) - 1),
        out_specs=(VMEM_SPEC,) * len(outs),
        scratch_shapes=[pltpu.VMEM((wide + rest, wide), jnp.float32)],
        compiler_params=pltpu.CompilerParams(vmem_limit_bytes=LIMIT),
        cost_estimate=cost(2 * (wide + rest) * wide * wide * 2),
        name="solve",
    )(*args)


def update_kernel(rows_n, target, first_row, terms, high, *refs):
    me_ref, one_ref, two_ref, got_ref = refs[:4]
    count = len(terms)
    left_refs = refs[4:4 + count]
    right_refs = refs[4 + count:4 + count + count * rows_n]
    outs = refs[4 + count + count * rows_n:-6]
    acc, left, right, raw, sem, raw_sem = refs[-6:]
    me, col = me_ref[0], me_ref[1]
    wide = rows_n * NB
    half = wide // 2
    height = high * NB
    pending = []
    theirs = pltpu.make_async_copy(got_ref.at[pl.ds(first_row - target, high)], raw.at[1], raw_sem.at[1])
    theirs.start()
    for i, (left_lo, right_los) in enumerate(terms):
        copies = [pltpu.make_async_copy(left_refs[i].at[pl.ds(left_lo, height), :], left.at[i], sem.at[i, rows_n])]
        for k in range(rows_n):
            lo = pl.multiple_of(lax.bitwise_xor(me, k) * NB, NB)
            copies.append(pltpu.make_async_copy(
                right_refs[i * rows_n + k].at[pl.ds(right_los[k], NB), :], right.at[i, pl.ds(lo, NB), :], sem.at[i, k]))
        for copy in copies:
            copy.start()
        pending.append(copies)
    for which, ref in ((0, one_ref), (1, two_ref)):
        @pl.when(col == which)
        def _(ref=ref):
            mine = pltpu.make_async_copy(
                ref.at[pl.ds(first_row, high), :, pl.ds(target * half, half)], raw.at[0], raw_sem.at[0])
            mine.start()
            mine.wait()
    theirs.wait()
    for q in range(rows_n // 2):
        cols = slice(q * NB, (q + 1) * NB)
        acc[:, pl.ds(pl.multiple_of((2 * q + col) * NB, NB), NB)] = raw[0, :, :, cols].reshape(height, NB)
        acc[:, pl.ds(pl.multiple_of((2 * q + 1 - col) * NB, NB), NB)] = raw[1, :, :, cols].reshape(height, NB)
    for i in range(count):
        for copy in pending[i]:
            copy.wait()
        acc[...] = acc[...] - nt(left[i], right[i])
    outs[0][...] = acc[:NB, :]
    if high > 1:
        outs[1][...] = acc[NB:, :]


def update(me, mats, got, target, first_row, high, lefts, rights, terms):
    rows_n = len(rights[0])
    wide = rows_n * NB
    height = high * NB
    count = len(terms)
    args = [me, *mats, got, *lefts, *[piece for group in rights for piece in group]]
    return pl.pallas_call(
        functools.partial(update_kernel, rows_n, target, first_row, terms, high),
        out_shape=(shape_of(NB, wide),) + ((shape_of(height - NB, wide),) if high > 1 else ()),
        in_specs=[SMEM_SPEC] + [HBM_SPEC] * (len(args) - 1),
        out_specs=(VMEM_SPEC,) * (2 if high > 1 else 1),
        scratch_shapes=[
            pltpu.VMEM((height, wide), jnp.float32),
            pltpu.VMEM((count, height, wide), jnp.float32),
            pltpu.VMEM((count, wide, wide), jnp.float32),
            pltpu.VMEM((2, high, NB, wide // 2), jnp.float32),
            pltpu.SemaphoreType.DMA((count, rows_n + 1)),
            pltpu.SemaphoreType.DMA((2,)),
        ],
        compiler_params=pltpu.CompilerParams(vmem_limit_bytes=LIMIT),
        cost_estimate=cost(2 * height * wide * wide * count * 2),
        name="update",
    )(*args)


def pick_kernel(cuts, me_ref, one_ref, two_ref, *refs):
    sem = refs[-1]
    for which, ref in ((0, two_ref), (1, one_ref)):
        @pl.when(me_ref[1] == which)
        def _(ref=ref):
            copies = [pltpu.make_async_copy(ref.at[pl.ds(lo, dst.shape[0]), :, pl.ds(col, dst.shape[2])], dst, sem.at[i])
                      for i, ((lo, col), dst) in enumerate(zip(cuts, refs[:-1]))]
            for copy in copies:
                copy.start()
            for copy in copies:
                copy.wait()


def pick(me, mats, cuts, width):
    rows = mats[0].shape[0]
    return pl.pallas_call(
        functools.partial(pick_kernel, cuts),
        out_shape=tuple(shape_of(rows - lo, NB, width) for lo, _ in cuts),
        in_specs=[SMEM_SPEC, HBM_SPEC, HBM_SPEC],
        out_specs=(VMEM_SPEC,) * len(cuts),
        scratch_shapes=[pltpu.SemaphoreType.DMA((len(cuts),))],
        compiler_params=pltpu.CompilerParams(vmem_limit_bytes=LIMIT),
        name="pick",
    )(me, *mats)


def place_kernel(steps, *refs):
    me_ref = refs[0]
    kept_refs, got_refs = refs[1:1 + steps], refs[1 + steps:1 + 2 * steps]
    one_ref, two_ref, sem = refs[1 + 2 * steps:]
    now, col = pl.program_id(0), me_ref[1]
    for i in range(steps):
        for which, dst_kept, dst_got in ((0, one_ref, two_ref), (1, two_ref, one_ref)):
            @pl.when(jnp.logical_and(now == i, col == which))
            def _(i=i, dst_kept=dst_kept, dst_got=dst_got):
                rows = pl.ds(i * NB, (steps - i) * NB)
                copies = [pltpu.make_async_copy(kept_refs[i], dst_kept.at[rows, :], sem.at[0]),
                          pltpu.make_async_copy(got_refs[i], dst_got.at[rows, :], sem.at[1])]
                for copy in copies:
                    copy.start()
                if i:
                    dst_kept[:i * NB, :] = jnp.zeros((i * NB, dst_kept.shape[1]), jnp.float32)
                    dst_got[:i * NB, :] = jnp.zeros((i * NB, dst_got.shape[1]), jnp.float32)
                for copy in copies:
                    copy.wait()


def place(me, kept, got):
    steps = len(kept)
    half = kept[0].shape[1]
    spec = pl.BlockSpec((steps * NB, half), lambda i: (0, i))
    return pl.pallas_call(
        functools.partial(place_kernel, steps),
        grid=(steps,),
        out_shape=(shape_of(steps * NB, steps * half),) * 2,
        in_specs=[SMEM_SPEC] + [HBM_SPEC] * (2 * steps),
        out_specs=(spec, spec),
        scratch_shapes=[pltpu.SemaphoreType.DMA((2,))],
        name="place",
    )(me, *kept, *got)


def tie(first, second):
    return lax.optimization_barrier((first, second))


def factor_pair(mat_one, mat_two, rows_n, cols_n):
    row_blocks, _, _ = mat_one.shape
    steps = row_blocks
    wide = rows_n * NB
    half = wide // cols_n
    per = half // NB
    my_row = lax.axis_index("row")
    my_col = lax.axis_index("col")
    first = my_col == 0
    me = jnp.stack([my_row, my_col]).astype(jnp.int32)
    swap = [(0, 1), (1, 0)]

    def hop(value, mask):
        return lax.ppermute(value, "row", [(i, i ^ mask) for i in range(rows_n)])

    def gather(value):
        return [value] + [hop(value, k) for k in range(1, rows_n)]

    def over_col(value):
        return lax.ppermute(value, "col", swap)

    def swapped(step, row_lo, after=None):
        cols = slice(step * half, (step + 1) * half)
        mask = first if after is None else tie(after, first)[1]
        return over_col(jnp.where(mask, mat_two[row_lo:, :, cols], mat_one[row_lo:, :, cols]))

    def panel_of(step, row_lo, row_hi, after=None, ready=None):
        cols = slice(step * half, (step + 1) * half)
        piece_one, piece_two = mat_one[row_lo:row_hi, :, cols], mat_two[row_lo:row_hi, :, cols]
        mask = first if after is None else tie(after, first)[1]
        got = over_col(jnp.where(mask, piece_two, piece_one)) if ready is None else over_col(ready)
        parts = []
        for q in range(per):
            cut = slice(q * NB, (q + 1) * NB)
            mine = jnp.where(first, piece_one[..., cut], piece_two[..., cut])
            parts += [jnp.where(first, mine, got[..., cut]), jnp.where(first, got[..., cut], mine)]
        return jnp.concatenate(parts, axis=-1).reshape(-1, wide), got

    def in_order(rel):
        picked = []
        for q in range(rows_n):
            value = rel[rows_n - 1]
            for k in range(rows_n - 1):
                value = jnp.where(my_row == (q ^ k), rel[k], value)
            picked.append(value)
        return jnp.concatenate(picked, axis=0)

    top, top_got = panel_of(0, 0, 1)
    chain_args = (in_order(gather(top)),)
    sub_own, _ = panel_of(0, 1, 2, top_got)
    diag_own, _ = panel_of(1, 1, 2, top_got)
    _, me_early = tie(top_got, me)
    low_send, rest_send = pick(me_early, (mat_one, mat_two), ((2, 0), (2, half)), half)
    low_own, _ = panel_of(0, 2, steps, ready=low_send)
    rest_own, _ = panel_of(1, 2, steps, ready=rest_send)
    own = jnp.concatenate([sub_own, low_own], axis=0)
    sub_rel, sub_lo = gather(sub_own), 0
    swaps = {}
    lowns, near, later, waiting = [], [], [], {}
    kept, sent = [], []

    for step in range(steps):
        lss, inv = chain(*chain_args)
        for ask in (2, 3) if step == 0 else (step + 3,):
            if ask < steps:
                swaps[ask] = swapped(ask, ask, lss)
        if step >= 2:
            lss, sent[step - 2] = tie(lss, sent[step - 2])
        if step - 2 in waiting:
            lss, far = tie(lss, waiting[step - 2])
            later[step - 2] = [later[step - 2][0], later[step - 2][1], far, hop(far, 1)]
        if step == steps - 1:
            full = lax.dynamic_slice(lss, (my_row * NB, 0), (NB, wide)).reshape(NB, per, cols_n, NB)
            even, odd = full[:, :, 0].reshape(NB, half), full[:, :, 1].reshape(NB, half)
            kept.append(jnp.where(first, even, odd))
            sent.append(lax.ppermute(jnp.where(first, odd, even), "col", swap))
            break
        target = step + 1
        if step >= 1:
            lefts, rights, terms_diag = [], [], []
            for past in range(step):
                base = (target - past - 1) * NB
                lefts.append(lowns[past])
                if past == step - 1:
                    rights.append(near[past])
                    los = (0,) * rows_n
                else:
                    rights.append(later[past])
                    los = ((target - past - 3) * NB,) * rows_n
                terms_diag.append((base, los))
            got = swaps[target]
            lss, me_now = tie(lss, me)
            parts = update(me_now, (mat_one, mat_two), got, target, target, steps - target, lefts, rights, terms_diag)
            diag_own, rest_own = parts if len(parts) > 1 else (parts[0], None)
        next_rel = gather(diag_own)
        if step - 1 < len(later) and step >= 1:
            _, value = tie(diag_own, later[step - 1])
            waiting[step - 1] = hop(value, 2)
            later[step - 1] = [value, hop(value, 1)]
        res = solve(me, lss, inv, own, sub_rel, sub_lo, rest_own)
        lown, chain_args = res[0], (me, res[1], *next_rel)
        lowns.append(lown)
        kept.append(res[2])
        sent.append(over_col(res[3]))
        if rest_own is not None:
            own = res[4]
            near.append(gather(res[5]))
            sub_rel, sub_lo = near[-1], NB
        if len(res) > 6:
            later.append(res[6])
    out_one, out_two = place(me, kept, sent)
    return out_one.reshape(mat_one.shape), out_two.reshape(mat_two.shape)


def solution(mesh):
    rows_n = mesh.shape["row"]
    cols_n = mesh.shape["col"]
    block_spec = P(("part", "row"), None, "col")

    def run_pair(mat_one, mat_two):
        return factor_pair(mat_one, mat_two, rows_n, cols_n)

    return jax.shard_map(run_pair, mesh=mesh, in_specs=(block_spec, block_spec), out_specs=(block_spec, block_spec), check_vma=False)
```
